16 devices in a mesh: sp: 16 (over z, y, x, core).
Axes of the slice: x: 2, y: 2, z: 2, core: 2. Of those that a mesh axis runs over, the one named last changes fastest.
Arguments:
- x_in: bfloat16 [8, 1024, 4096], P(None, 'sp')
- dy_in: bfloat16 [8, 1024, 4096], P(None, 'sp')
- w_qkv: bfloat16 [4096, 8, 6, 128], replicated
- w_out: bfloat16 [4096, 4096], replicated
- ln_gain: float32 [4096], replicated
- ln_bias: float32 [4096], replicated
- positions: int32 [1024], P('sp')
Outputs:
- output 1: bfloat16 [8, 1024, 4096], P(None, 'sp')
- output 2: bfloat16 [8, 1024, 4096], P(None, 'sp')
- output 3: float32 [4096, 8, 6, 128], replicated
- output 4: float32 [4096, 4096], replicated
- output 5: float32 [4096], replicated
- output 6: float32 [4096], replicated
All inputs are finite; a program needn't handle non-finite values.
Results may differ from the reference program's by a relative error of at most 0.0153087.
Values are sent between devices in bfloat16 or wider.
A program may use at most 1.25 GiB of HBM per device.

```python
import functools
import jax
import jax.numpy as jnp
from jax import lax

D = 4096
HEADS = 32
KV_HEADS = 8
HEAD = 128
BATCH = 8
SEQ = 1024
GROUP_Q = HEADS // KV_HEADS
QKV_COLS = KV_HEADS * (GROUP_Q + 2) * HEAD
SCORE_SCALE = HEAD ** -0.5
QKV_SCALE = 1.5 * D ** -0.5
OUT_SCALE = (HEADS * HEAD) ** -0.5
LN_EPS = 1e-5
ROPE_BASE = 10000.0


def setup_inputs(seed: int = 0) -> dict:
    base_key = jax.random.key(seed)
    key_x, key_dy, key_qkv, key_out, key_gain, key_bias, key_pos = jax.random.split(base_key, 7)
    x_in = jax.random.normal(key_x, (BATCH, SEQ, D), jnp.float32).astype(jnp.bfloat16)
    dy_in = jax.random.normal(key_dy, (BATCH, SEQ, D), jnp.float32).astype(jnp.bfloat16)
    w_qkv = (jax.random.normal(key_qkv, (D, KV_HEADS, GROUP_Q + 2, HEAD), jnp.float32) * QKV_SCALE).astype(jnp.bfloat16)
    w_out = (jax.random.normal(key_out, (HEADS * HEAD, D), jnp.float32) * OUT_SCALE).astype(jnp.bfloat16)
    ln_gain = 1.0 + 0.3 * jax.random.normal(key_gain, (D,), jnp.float32)
    ln_bias = 0.3 * jax.random.normal(key_bias, (D,), jnp.float32)
    pos_steps = jax.random.randint(key_pos, (SEQ,), 1, 4)
    positions = (jnp.cumsum(pos_steps) - pos_steps[0]).astype(jnp.int32)
    return {'x_in': x_in, 'dy_in': dy_in, 'w_qkv': w_qkv, 'w_out': w_out, 'ln_gain': ln_gain, 'ln_bias': ln_bias, 'positions': positions}


def layer_norm(x_rows, ln_gain, ln_bias):
    x_f32 = x_rows.astype(jnp.float32)
    centered = x_f32 - jnp.mean(x_f32, axis=-1, keepdims=True)
    variance = jnp.mean(centered * centered, axis=-1, keepdims=True)
    return (centered * lax.rsqrt(variance + LN_EPS) * ln_gain + ln_bias).astype(jnp.bfloat16)


def rope_tables(positions):
    exponents = jnp.arange(HEAD // 2, dtype=jnp.float32) * (2.0 / HEAD)
    inv_freq = jnp.power(ROPE_BASE, -exponents)
    angles = positions.astype(jnp.float32)[:, None] * inv_freq[None, :]
    return jnp.cos(angles), jnp.sin(angles)


def rotate(t_in, cos_tab, sin_tab):
    half_dim = t_in.shape[-1] // 2
    t_f32 = t_in.astype(jnp.float32)
    first_half = t_f32[..., :half_dim]
    second_half = t_f32[..., half_dim:]
    cos_b = cos_tab[None, :, None, :]
    sin_b = sin_tab[None, :, None, :]
    return jnp.concatenate([first_half * cos_b - second_half * sin_b, second_half * cos_b + first_half * sin_b], axis=-1).astype(jnp.bfloat16)


def attention_core(qkv_act, cos_tab, sin_tab):
    q_rot = rotate(qkv_act[:, :, :, :GROUP_Q, :].reshape(BATCH, SEQ, HEADS, HEAD), cos_tab, sin_tab)
    k_rot = rotate(qkv_act[:, :, :, GROUP_Q, :], cos_tab, sin_tab)
    v_val = qkv_act[:, :, :, GROUP_Q + 1, :]
    q_all = jnp.moveaxis(q_rot.astype(jnp.float32), 2, 0)
    k_all = jnp.moveaxis(jnp.repeat(k_rot.astype(jnp.float32), GROUP_Q, axis=2), 2, 0)
    v_all = jnp.moveaxis(jnp.repeat(v_val.astype(jnp.float32), GROUP_Q, axis=2), 2, 0)
    causal = jnp.arange(SEQ)[:, None] >= jnp.arange(SEQ)[None, :]

    def one_head(operands):
        q_head, k_head, v_head = operands
        scores = jnp.einsum('bqh,bkh->bqk', q_head, k_head) * SCORE_SCALE
        attn_probs = jax.nn.softmax(jnp.where(causal, scores, -jnp.inf), axis=-1)
        probs_b = attn_probs.astype(jnp.bfloat16).astype(jnp.float32)
        return jnp.einsum('bqk,bkh->bqh', probs_b, v_head).astype(jnp.bfloat16)

    head_ctx = lax.map(jax.checkpoint(one_head), (q_all, k_all, v_all))
    return jnp.moveaxis(head_ctx, 0, 2).reshape(BATCH, SEQ, HEADS * HEAD)


def reference(x_in, dy_in, w_qkv, w_out, ln_gain, ln_bias, positions):
    cos_tab, sin_tab = rope_tables(positions)
    h_norm, ln_back = jax.vjp(layer_norm, x_in, ln_gain, ln_bias)
    h_rows = h_norm.reshape(BATCH * SEQ, D)
    w_rows = w_qkv.reshape(D, QKV_COLS)
    qkv_act = jnp.dot(h_rows, w_rows, preferred_element_type=jnp.float32).astype(jnp.bfloat16)
    qkv_act = qkv_act.reshape(BATCH, SEQ, KV_HEADS, GROUP_Q + 2, HEAD)
    context, core_back = jax.vjp(functools.partial(attention_core, cos_tab=cos_tab, sin_tab=sin_tab), qkv_act)
    ctx_rows = context.reshape(BATCH * SEQ, HEADS * HEAD)
    dy_rows = dy_in.reshape(BATCH * SEQ, D)
    attn_out = jnp.dot(ctx_rows, w_out, preferred_element_type=jnp.float32).astype(jnp.bfloat16).reshape(BATCH, SEQ, D)
    grad_w_out = jnp.dot(ctx_rows.T, dy_rows, preferred_element_type=jnp.float32)
    grad_ctx = jnp.dot(dy_rows, w_out.T, preferred_element_type=jnp.float32).astype(jnp.bfloat16)
    (grad_qkv,) = core_back(grad_ctx.reshape(BATCH, SEQ, HEADS * HEAD))
    grad_rows = grad_qkv.reshape(BATCH * SEQ, QKV_COLS)
    grad_w_qkv = jnp.dot(h_rows.T, grad_rows, preferred_element_type=jnp.float32).reshape(D, KV_HEADS, GROUP_Q + 2, HEAD)
    grad_h = jnp.dot(grad_rows, w_rows.T, preferred_element_type=jnp.float32).astype(jnp.bfloat16).reshape(BATCH, SEQ, D)
    grad_x, grad_gain, grad_bias = ln_back(grad_h)
    return attn_out, grad_x, grad_w_qkv, grad_w_out, grad_gain, grad_bias
```

```python
import functools

import jax
import jax.numpy as jnp
from jax import lax
from jax.experimental import pallas as pl
from jax.experimental.pallas import tpu as pltpu
from jax.sharding import PartitionSpec as P


LN_EPS = 1e-5
ROPE_BASE = 10000.0
F32 = jnp.float32
BF16 = jnp.bfloat16
QB = 256


def layer_norm(x_rows, ln_gain, ln_bias):
    x_f32 = x_rows.astype(F32)
    centered = x_f32 - jnp.mean(x_f32, axis=-1, keepdims=True)
    variance = jnp.mean(centered * centered, axis=-1, keepdims=True)
    return (centered * lax.rsqrt(variance + LN_EPS) * ln_gain + ln_bias).astype(BF16)


def rope_tables(positions, head_dim):
    exponents = jnp.arange(head_dim // 2, dtype=F32) * (2.0 / head_dim)
    inv_freq = jnp.power(ROPE_BASE, -exponents)
    angles = positions.astype(F32)[:, None] * inv_freq[None, :]
    cos_half, sin_half = jnp.cos(angles), jnp.sin(angles)
    return jnp.concatenate([cos_half, cos_half], axis=-1), jnp.concatenate([-sin_half, sin_half], axis=-1)


def rotate(t_in, cos_full, sin_signed):
    t_f32 = t_in.astype(F32)
    half_dim = t_in.shape[-1] // 2
    swapped = jnp.concatenate([t_f32[..., half_dim:], t_f32[..., :half_dim]], axis=-1)
    return (t_f32 * cos_full + swapped * sin_signed).astype(BF16)


def rotate_rows(t_in, cos_full, sin_signed):
    t_f32 = t_in.astype(F32)
    swapped = pltpu.roll(t_f32, t_in.shape[-1] // 2, 1)
    return (t_f32 * cos_full + swapped * sin_signed).astype(BF16)


def dot(a, b, dims):
    return lax.dot_general(a, b, (dims, ((), ())), preferred_element_type=F32)


def masked_scores(k_rot, q_rot, block, scale):
    keys = (block + 1) * QB
    scores = dot(k_rot[:keys], q_rot[block * QB:keys], ((1,), (1,))) * scale
    key_id = lax.broadcasted_iota(jnp.int32, (QB, QB), 0)
    query_id = lax.broadcasted_iota(jnp.int32, (QB, QB), 1)
    diag = jnp.where(key_id <= query_id, scores[block * QB:], -jnp.inf)
    return jnp.concatenate([scores[:block * QB], diag], axis=0) if block else diag


def attn_fwd_kernel(q_ref, k_ref, v_ref, cos_ref, sin_ref, ctx_ref, qr_ref, kr_ref, max_ref, sum_ref, turn_ref, *, scale):
    chunks, _, rows, head_dim = q_ref.shape
    seq = chunks * rows
    cos_full, sin_signed = cos_ref[...], sin_ref[...]
    q_rot = rotate_rows(q_ref[...].reshape(seq, head_dim), cos_full, sin_signed)
    k_rot = rotate_rows(k_ref[...].reshape(seq, head_dim), cos_full, sin_signed)
    qr_ref[...] = q_rot.reshape(q_ref.shape)
    kr_ref[...] = k_rot.reshape(q_ref.shape)
    v_t = v_ref[...].reshape(seq, head_dim).T
    per = QB // rows
    for block in range(seq // QB):
        keys = (block + 1) * QB
        scores = masked_scores(k_rot, q_rot, block, scale)
        row_max = jnp.max(scores, axis=0, keepdims=True)
        expd = jnp.exp(scores - row_max)
        row_sum = jnp.sum(expd, axis=0, keepdims=True)
        probs = (expd * (1.0 / row_sum)).astype(BF16)
        turn_ref[...] = dot(v_t[:, :keys], probs, ((1,), (0,)))
        ctx = turn_ref[...].T.astype(BF16)
        ctx_ref[block * per:(block + 1) * per] = ctx.reshape(per, 1, rows, head_dim)
        max_ref[0, 0, :, block * QB:keys] = row_max
        sum_ref[0, 0, :, block * QB:keys] = row_sum


def attn_bwd_kernel(q_ref, k_ref, v_ref, g_ref, cos_ref, sin_ref, max_ref, sum_ref, gq_ref, gk_ref, gv_ref, gk_acc, gv_acc, turn_ref, *, scale):
    chunks, _, rows, head_dim = q_ref.shape
    seq = chunks * rows
    head = pl.program_id(1)
    q_rot = q_ref[...].reshape(seq, head_dim)
    k_rot = k_ref[...].reshape(seq, head_dim)
    v_val = v_ref[...].reshape(seq, head_dim)
    g_val = g_ref[...].reshape(seq, head_dim)
    k_t = k_rot.T
    per = QB // rows

    @pl.when(head == 0)
    def _():
        gk_acc[...] = jnp.zeros_like(gk_acc)
        gv_acc[...] = jnp.zeros_like(gv_acc)

    for block in range(seq // QB):
        keys = (block + 1) * QB
        span = slice(block * QB, keys)
        scores = masked_scores(k_rot, q_rot, block, scale)
        probs = jnp.exp(scores - max_ref[0, 0, :, span]) * (1.0 / sum_ref[0, 0, :, span])
        g_blk = g_val[span]
        gv_acc[:keys] += dot(probs.astype(BF16), g_blk, ((1,), (0,)))
        grad_probs = dot(v_val[:keys], g_blk, ((1,), (1,))).astype(BF16).astype(F32)
        row_dot = jnp.sum(grad_probs * probs, axis=0, keepdims=True)
        grad_scores = (probs * (grad_probs - row_dot) * scale).astype(BF16)
        gk_acc[:keys] += dot(grad_scores, q_rot[span], ((1,), (0,)))
        turn_ref[...] = dot(k_t[:, :keys], grad_scores, ((1,), (0,)))
        gq = rotate_rows(turn_ref[...].T.astype(BF16), cos_ref[span], -sin_ref[span])
        gq_ref[block * per:(block + 1) * per] = gq.reshape(per, 1, rows, head_dim)

    @pl.when(head == pl.num_programs(1) - 1)
    def _():
        gk_ref[...] = gk_acc[...].astype(BF16).reshape(gk_ref.shape)
        gv_ref[...] = gv_acc[...].astype(BF16).reshape(gv_ref.shape)


def attn_specs(chunks, rows, head_dim):
    seq = chunks * rows
    blk = (chunks, 1, rows, head_dim)
    per_head = pl.BlockSpec(blk, lambda b, h: (0, b, 0, h))
    col = lambda c: pl.BlockSpec(blk, lambda b, h: (0, b, 0, c))
    table = pl.BlockSpec((seq, head_dim), lambda b, h: (0, 0))
    stat = pl.BlockSpec((1, 1, 1, seq), lambda b, h: (b, h, 0, 0))
    return per_head, col, table, stat


def attn_params(batch, heads, seq, head_dim, dots, name):
    flops = batch * heads * dots * seq * seq * head_dim
    return dict(
        cost_estimate=pl.CostEstimate(flops=flops, bytes_accessed=batch * seq * head_dim * 20, transcendentals=batch * heads * seq * seq // 2),
        compiler_params=pltpu.CompilerParams(dimension_semantics=("arbitrary", "arbitrary"), vmem_limit_bytes=48 * 2**20),
        name=name,
    )


def attn_fwd(qkv, cos_full, sin_signed, heads, scale):
    chunks, batch, rows, width = qkv.shape
    head_dim = width // (heads + 2)
    seq = chunks * rows
    per_head, col, table, stat = attn_specs(chunks, rows, head_dim)
    out = lambda n: jax.ShapeDtypeStruct((chunks, batch, rows, n * head_dim), BF16)
    stats = jax.ShapeDtypeStruct((batch, heads, 1, seq), F32)
    return pl.pallas_call(
        functools.partial(attn_fwd_kernel, scale=scale),
        grid=(batch, heads),
        in_specs=[per_head, col(heads), col(heads + 1), table, table],
        out_specs=[per_head, per_head, col(0), stat, stat],
        out_shape=[out(heads), out(heads), out(1), stats, stats],
        scratch_shapes=[pltpu.VMEM((head_dim, QB), F32)],
        **attn_params(batch, heads, seq, head_dim, 2, "attn_fwd"),
    )(qkv, qkv, qkv, cos_full, sin_signed)


def attn_bwd(q_rot, k_rot, qkv, grad_ctx, cos_full, sin_signed, row_max, row_sum, heads, scale):
    chunks, batch, rows, width = qkv.shape
    head_dim = width // (heads + 2)
    seq = chunks * rows
    per_head, col, table, stat = attn_specs(chunks, rows, head_dim)
    out = lambda n: jax.ShapeDtypeStruct((chunks, batch, rows, n * head_dim), BF16)
    return pl.pallas_call(
        functools.partial(attn_bwd_kernel, scale=scale),
        grid=(batch, heads),
        in_specs=[per_head, col(0), col(heads + 1), per_head, table, table, stat, stat],
        out_specs=[per_head, col(0), col(0)],
        out_shape=[out(heads), out(1), out(1)],
        scratch_shapes=[pltpu.VMEM((seq, head_dim), F32), pltpu.VMEM((seq, head_dim), F32), pltpu.VMEM((head_dim, QB), F32)],
        **attn_params(batch, heads, seq, head_dim, 5, "attn_bwd"),
    )(q_rot, k_rot, qkv, grad_ctx, cos_full, sin_signed, row_max, row_sum)


def device_slots(device, group_q):
    core, half = device % 2, group_q // 2
    return [core * half + n for n in range(half)] + [group_q + core]


def place_kernel(part_ref, old_ref, out_ref, *, kv_heads, group_q):
    del old_ref
    devices, rows, _ = part_ref.shape
    head_dim = out_ref.shape[1]
    slots = group_q + 2
    for device in range(devices):
        for n, slot in enumerate(device_slots(device, group_q)):
            out_ref[pl.ds(slot * kv_heads + device // 2, rows, slots * kv_heads), :] = part_ref[device, :, n * head_dim:(n + 1) * head_dim]


def split_kernel(w_ref, dev_ref, wide_ref, *, kv_heads, group_q):
    devices, rows, _ = dev_ref.shape
    head_dim = w_ref.shape[1]
    slots = group_q + 2
    wide_ref[...] = w_ref[...].astype(F32)
    for device in range(devices):
        for n, slot in enumerate(device_slots(device, group_q)):
            picked = wide_ref[pl.ds(slot * kv_heads + device // 2, rows, slots * kv_heads), :]
            dev_ref[device, :, n * head_dim:(n + 1) * head_dim] = picked.astype(BF16)


def split(w_flat, width, devices, kv_heads, group_q):
    slots, head_dim = (group_q + 2) * kv_heads, w_flat.shape[1]
    blk = 64
    cols = (group_q // 2 + 1) * head_dim
    return pl.pallas_call(
        functools.partial(split_kernel, kv_heads=kv_heads, group_q=group_q),
        grid=(width // blk,),
        in_specs=[pl.BlockSpec((blk * slots, head_dim), lambda i: (i, 0))],
        out_specs=pl.BlockSpec((devices, blk, cols), lambda i: (0, i, 0)),
        out_shape=jax.ShapeDtypeStruct((devices, width, cols), BF16),
        scratch_shapes=[pltpu.VMEM((blk * slots, head_dim), F32)],
        cost_estimate=pl.CostEstimate(flops=width * slots * head_dim * 2000, bytes_accessed=4 * width * slots * head_dim, transcendentals=0),
        compiler_params=pltpu.CompilerParams(dimension_semantics=("arbitrary",), vmem_limit_bytes=48 * 2**20),
        name="split",
    )(w_flat)


def place(part, old, index, pieces, kv_heads, group_q):
    devices, rows, width = part.shape
    head_dim = width // (group_q // 2 + 1)
    slots = (group_q + 2) * kv_heads
    blk = 64
    steps = rows // blk
    out_shape = jax.ShapeDtypeStruct((pieces * rows * slots, head_dim), F32)
    kernel = functools.partial(place_kernel, kv_heads=kv_heads, group_q=group_q)
    in_specs = [pl.BlockSpec((devices, blk, width), lambda i: (0, i, 0))]
    args = [part]
    alias = {}
    if old is None:
        kernel_fn = lambda part_ref, out_ref: kernel(part_ref, None, out_ref)
    else:
        kernel_fn = kernel
        in_specs.append(pl.BlockSpec(memory_space=pl.ANY))
        args.append(old)
        alias = {1: 0}
    return pl.pallas_call(
        kernel_fn,
        grid=(steps,),
        in_specs=in_specs,
        out_specs=pl.BlockSpec((blk * slots, head_dim), lambda i: (index * steps + i, 0)),
        out_shape=out_shape,
        input_output_aliases=alias,
        cost_estimate=pl.CostEstimate(flops=rows * slots * head_dim * 2000, bytes_accessed=2 * 4 * rows * slots * head_dim, transcendentals=0),
        compiler_params=pltpu.CompilerParams(dimension_semantics=("arbitrary",), vmem_limit_bytes=48 * 2**20),
        name="place",
    )(*args)


def copy(array):
    rows, width = array.shape
    blk = pl.BlockSpec((256, width), lambda i: (i, 0))

    def kernel(in_ref, out_ref):
        out_ref[...] = in_ref[...]

    return pl.pallas_call(
        kernel,
        grid=(rows // 256,),
        in_specs=[blk],
        out_specs=blk,
        out_shape=jax.ShapeDtypeStruct(array.shape, array.dtype),
        cost_estimate=pl.CostEstimate(flops=rows * width * 2000, bytes_accessed=8 * rows * width, transcendentals=0),
        compiler_params=pltpu.CompilerParams(dimension_semantics=("arbitrary",), vmem_limit_bytes=48 * 2**20),
    )(array)


def solution(mesh):
    sp_size = mesh.shape['sp']
    seq_spec = P(None, 'sp', None)
    pieces = 4

    def per_device(x_loc, dy_loc, w_qkv, w_out, ln_gain, ln_bias, pos_loc):
        batch, seq_loc, width = x_loc.shape
        kv_heads, head_dim = w_qkv.shape[1], w_qkv.shape[3]
        group_q = w_qkv.shape[2] - 2
        heads = kv_heads * group_q // sp_size
        scale = head_dim ** -0.5
        me = lax.axis_index('sp')
        group, core = me // 2, me % 2
        own_w = heads * head_dim

        h_norm, ln_back = jax.vjp(layer_norm, x_loc, ln_gain, ln_bias)
        h_all = lax.all_gather(h_norm, 'sp')
        dy_all = lax.all_gather(dy_loc, 'sp')
        pos_all = lax.all_gather(pos_loc, 'sp', tiled=True)
        cos_full, sin_signed = rope_tables(pos_all, head_dim)

        w_dev = split(w_qkv.transpose(0, 2, 1, 3).reshape(-1, head_dim), width, sp_size, kv_heads, group_q)
        pair = lax.dynamic_slice(w_dev, (2 * group, 0, own_w), (2, width, head_dim))
        w_own = jnp.concatenate([lax.dynamic_slice(w_dev, (me, 0, 0), (1, width, own_w))[0], pair[0], pair[1]], axis=-1)
        w_out_own = lax.dynamic_slice(w_out, (me * own_w, 0), (own_w, width))

        tokens = sp_size * batch * seq_loc
        by_chunk = lambda t: t.reshape(sp_size, batch, seq_loc, t.shape[-1])
        flat = lambda t: t.reshape(tokens, t.shape[-1])
        h_rows, dy_rows = flat(h_all), flat(dy_all)

        qkv = by_chunk(dot(h_rows, w_own, ((1,), (0,))).astype(BF16))
        ctx, q_rot, k_rot, row_max, row_sum = attn_fwd(qkv, cos_full, sin_signed, heads, scale)
        ctx_got = lax.all_to_all(ctx, 'sp', 0, 0)

        grad_w_out_own = dot(flat(ctx), dy_rows, ((0,), (0,)))
        grad_w_out = copy(lax.all_gather(grad_w_out_own, 'sp', tiled=True))

        grad_ctx = jnp.einsum('ibsd,cd->ibsc', dy_all, w_out_own, preferred_element_type=F32).astype(BF16)
        grad_ctx, grad_w_out_own = lax.optimization_barrier((grad_ctx, grad_w_out_own))
        grad_q, grad_k_part, grad_v_part = attn_bwd(q_rot, k_rot, qkv, grad_ctx, cos_full, sin_signed, row_max, row_sum, heads, scale)
        kept = jnp.where(core == 0, grad_k_part, grad_v_part)
        sent = jnp.where(core == 0, grad_v_part, grad_k_part)
        got = lax.ppermute(sent, 'sp', [(i, i ^ 1) for i in range(sp_size)])
        grad_kv = (kept.astype(F32) + got.astype(F32)).astype(BF16)
        pos_of = lambda table: table.reshape(sp_size, 1, seq_loc, head_dim)
        grad_kv = jnp.where(core == 0, rotate(grad_kv, pos_of(cos_full), pos_of(-sin_signed)), grad_kv)
        grad_own = jnp.concatenate([grad_q, grad_kv], axis=-1)
        grad_got = lax.all_to_all(grad_own, 'sp', 0, 0)

        rows = width // pieces
        grad_w_own = dot(h_rows, flat(grad_own), ((0,), (0,)))
        grad_w = None
        for n in range(pieces):
            part = lax.all_gather(grad_w_own[n * rows:(n + 1) * rows], 'sp')
            grad_w = place(part, grad_w, n, pieces, kv_heads, group_q)
        grad_w_qkv = grad_w.reshape(width, group_q + 2, kv_heads, head_dim).transpose(0, 2, 1, 3)

        attn_out = jnp.einsum('ibsc,icd->bsd', ctx_got, w_out.reshape(sp_size, own_w, width), preferred_element_type=F32).astype(BF16)
        grad_h = jnp.einsum('ibsc,idc->bsd', grad_got, w_dev, preferred_element_type=F32).astype(BF16)
        grad_x, grad_gain, grad_bias = ln_back(grad_h)
        grad_gain, grad_bias = lax.psum((grad_gain, grad_bias), 'sp')
        return attn_out, grad_x, grad_w_qkv, grad_w_out, grad_gain, grad_bias

    return jax.shard_map(per_device, mesh=mesh, in_specs=(seq_spec, seq_spec, P(), P(), P(), P(), P('sp')), out_specs=(seq_spec, seq_spec, P(), P(), P(), P()), check_vma=False)
```
